32 devices in a mesh: dom: 8 (over z, x), sub: 4 (over y, core).
Axes of the slice: x: 2, y: 2, z: 4, core: 2. Of those that a mesh axis runs over, the one named last changes fastest.
Arguments:
- primitive: float32 [5, 65536], P(None, ('dom', 'sub')), may hold values from -3 to 3
- gradient: float32 [15, 65536], P(None, ('dom', 'sub')), may hold values from -1.5 to 1.5
- volume: float32 [65536], P(('dom', 'sub')), may hold values from 0.5 to 4
- face_left: int32 [196608], P(('dom', 'sub')), may hold values from 0 to 2047
- face_right: int32 [196608], P(('dom', 'sub')), may hold values from 0 to 4095, as said below
- face_angles: float32 [2, 196608], P(None, ('dom', 'sub')), may hold values from -3.140625 to 3.140625
- face_area: float32 [196608], P(('dom', 'sub')), may hold values from 0.2 to 2
- face_offsets: float32 [6, 196608], P(None, ('dom', 'sub')), may hold values from -1 to 1
- rim_left: int32 [16384], P(('dom', 'sub')), may hold values from 0 to 511
- rim_right: int32 [16384], P(('dom', 'sub')), may hold values from 0 to 511
- rim_angles: float32 [2, 16384], P(None, ('dom', 'sub')), may hold values from -3.140625 to 3.140625
- rim_area: float32 [16384], P(('dom', 'sub')), may hold values from 0.2 to 2
- rim_offsets: float32 [6, 16384], P(None, ('dom', 'sub')), may hold values from -1 to 1
- send_list: int32 [512], P(('dom', 'sub')), may hold values from -1 to 15, as said below
Outputs:
- change_rate: float32 [5, 65536], P(None, ('dom', 'sub'))
- new_conserved: float32 [5, 65536], P(None, ('dom', 'sub'))
- time_step: float32 [], replicated
The draws below stay inside these ranges and needn't reach their ends.
Inputs may be any that keep to these rules, and one draw needn't show every extreme that they name: `send_list`: an entry is a block number of the sending device or -1 for an unused slot; for each peer the used slots come first, at most 4 of them, a device sends no block to itself, and each device fills all 4 slots of one peer. `face_right`: an entry of at least 2048 names ghost cell (s * 4 + j) * 128 + k only where slot j of the sending peer s is used.
All inputs are finite; a program needn't handle non-finite values.
Results may differ from the reference program's by a relative error of at most 0.0003.
Values sent between devices are 32-bit elements; how exact they have to be, the bound alone decides.
A program may use at most 64 MiB of HBM per device.

```python
import math
import jax
import jax.numpy as jnp
from jax import lax

BLK = 128
NB = 16
RIM = 4
CAP = 4
FACES = 6144
NCELL = 65536
NFACE = 196608
NRIM = 16384
N_DOM = 8
N_SUB = 4
DEVICES = 32


def peer_counts(key):
    key_counts = jax.random.fold_in(key, 11)
    base_counts = jax.random.randint(key_counts, (DEVICES, N_SUB), 1, CAP + 1)
    source = jnp.arange(DEVICES, dtype=jnp.int32) % N_SUB
    target = jnp.arange(N_SUB, dtype=jnp.int32)
    full_peer = target[None, :] == (source[:, None] + 1) % N_SUB
    counts = jnp.where(full_peer, CAP, base_counts)
    return jnp.where(target[None, :] == source[:, None], 0, counts).astype(jnp.int32)


def draw_send_list(key, part):
    counts = peer_counts(key)
    block_ids = jax.random.randint(jax.random.fold_in(key, 12), (DEVICES, N_SUB, CAP), 0, NB)
    slot_index = jnp.arange(CAP, dtype=jnp.int32)
    chosen = jnp.where(slot_index[None, None, :] < counts[:, :, None], block_ids, -1)
    return chosen.reshape(-1).astype(jnp.int32)


def draw_face_right(key, part):
    counts = peer_counts(key)
    device = jnp.arange(DEVICES, dtype=jnp.int32)[:, None]
    dom_index = device // N_SUB
    sub_index = device % N_SUB
    local_pick = jax.random.randint(jax.random.fold_in(key, 21), (DEVICES, FACES), 0, NB * BLK)
    source = jax.random.randint(jax.random.fold_in(key, 22), (DEVICES, FACES), 0, N_SUB)
    available = counts[dom_index * N_SUB + source, sub_index]
    slot_index = jax.random.randint(jax.random.fold_in(key, 23), (DEVICES, FACES), 0, CAP) % jnp.maximum(available, 1)
    cell_index = jax.random.randint(jax.random.fold_in(key, 24), (DEVICES, FACES), 0, BLK)
    coin_flip = jax.random.randint(jax.random.fold_in(key, 25), (DEVICES, FACES), 0, 4)
    ghost_pick = NB * BLK + (source * CAP + slot_index) * BLK + cell_index
    chosen = jnp.where((coin_flip == 0) & (available > 0), ghost_pick, local_pick)
    return chosen.reshape(-1).astype(jnp.int32)


def set_ends(array, rng, smallest, largest):
    spot = [jax.random.randint(jax.random.fold_in(rng, axis), (), 0, length) for axis, length in enumerate(array.shape)]
    longest = array.shape.index(max(array.shape))
    next_to = spot[:longest] + [(spot[longest] + 1) % array.shape[longest]] + spot[longest + 1:]
    return array.at[tuple(spot)].set(smallest).at[tuple(next_to)].set(largest)


def levels(key, extent, shards, least, largest):
    def one(axis_at, blocks):
        draws = jax.random.uniform(jax.random.fold_in(jax.random.fold_in(key, 6), axis_at), (blocks,), jnp.float32, least / len(shards), largest / len(shards))
        return jnp.repeat(jnp.exp(draws), extent[axis_at] // blocks).reshape((-1,) + (1,) * (len(extent) - axis_at - 1))

    factor_of = one(*shards[0])
    for cut in shards[1:]:
        factor_of = factor_of * one(*cut)
    return factor_of


def centred(own_key, dims, scale, limit, pieces=(), kind=jnp.bfloat16):
    result = jax.random.normal(own_key, dims, jnp.float32) * scale
    if len(pieces) > 0:
        result = levels(own_key, dims, pieces, -0.22, 0.18) * result
    return jnp.clip(result, min=-limit, max=limit).astype(kind)


def setup_inputs(seed: int = 0) -> dict:
    keys = jax.random.split(jax.random.key(seed), 15)
    return {
        "primitive": centred(keys[0], (5, NCELL), 0.5, 3.0, ((1, 32),), jnp.float32),
        "gradient": centred(keys[1], (15, NCELL), 0.3, 1.5, ((1, 32),), jnp.float32),
        "volume": jnp.clip(jnp.exp(math.log(4.0) - 2.0794415 * jax.random.uniform(keys[2], (NCELL,), jnp.float32) ** levels(keys[2], (NCELL,), ((0, 32),), -0.2, 0.2)), 0.5, 4.0),
        "face_left": set_ends(jax.random.randint(keys[3], (NFACE,), 0, NB * BLK), jax.random.fold_in(keys[3], 1), 0, (NB * BLK) - 1).astype(jnp.int32),
        "face_right": draw_face_right(jax.random.fold_in(keys[14], 71), 0),
        "face_angles": jnp.clip(jax.random.uniform(keys[5], (2, NFACE), jnp.float32, -3.140625, 3.140625), -3.140625, 3.140625),
        "face_area": jnp.clip(jnp.exp(math.log(2.0) - 2.3025851 * jax.random.uniform(keys[6], (NFACE,), jnp.float32) ** levels(keys[6], (NFACE,), ((0, 32),), -0.2, 0.2)), 0.2, 2.0),
        "face_offsets": centred(keys[7], (6, NFACE), 0.3, 1.0, ((1, 32),), jnp.float32),
        "rim_left": set_ends(jax.random.randint(keys[8], (NRIM,), 0, RIM * BLK), jax.random.fold_in(keys[8], 1), 0, (RIM * BLK) - 1).astype(jnp.int32),
        "rim_right": set_ends(jax.random.randint(keys[9], (NRIM,), 0, RIM * BLK), jax.random.fold_in(keys[9], 1), 0, (RIM * BLK) - 1).astype(jnp.int32),
        "rim_angles": jnp.clip(jax.random.uniform(keys[10], (2, NRIM), jnp.float32, -3.140625, 3.140625), -3.140625, 3.140625),
        "rim_area": jnp.clip(jnp.exp(math.log(2.0) - 2.3025851 * jax.random.uniform(keys[11], (NRIM,), jnp.float32) ** levels(keys[11], (NRIM,), ((0, 32),), -0.2, 0.2)), 0.2, 2.0),
        "rim_offsets": centred(keys[12], (6, NRIM), 0.3, 1.0, ((1, 32),), jnp.float32),
        "send_list": draw_send_list(jax.random.fold_in(keys[14], 71), 0),
    }


adiabatic = 5.0 / 3.0
courant = 0.3

def face_states(side_cells, shifts):
    centre_values = side_cells[:5]
    slopes = side_cells[5:].reshape(5, 3, -1)
    values = centre_values + lax.optimization_barrier(jnp.sum(slopes * shifts[None], axis=1))
    return (jnp.exp(values[0]), values[1:4], jnp.exp(values[4]))

def conserved_flux(density, velocity, pressure, normal):
    normal_speed = lax.optimization_barrier(jnp.sum(velocity * normal, axis=0))
    energy = pressure / (adiabatic - 1.0) + 0.5 * density * lax.optimization_barrier(jnp.sum(velocity * velocity, axis=0))
    conserved = jnp.concatenate([density[None], density * velocity, energy[None]], 0)
    flux_vector = jnp.concatenate([(density * normal_speed)[None], density * velocity * normal_speed + pressure * normal, ((energy + pressure) * normal_speed)[None]], 0)
    return (normal_speed, energy, conserved, flux_vector)

def star_flux(density, velocity, pressure, normal, normal_speed, energy, conserved, flux_vector, signal, contact):
    mass_rate = density * (signal - normal_speed)
    factor = mass_rate / (signal - contact)
    star_state = factor * jnp.concatenate([jnp.ones_like(density)[None], velocity + (contact - normal_speed) * normal, (energy / density + (contact - normal_speed) * (contact + pressure / mass_rate))[None]], 0)
    return flux_vector + signal * (star_state - conserved)

def hllc_flux(left_cells, right_cells, angles, offsets):
    normal = jnp.stack([jnp.sin(angles[0]) * jnp.cos(angles[1]), jnp.sin(angles[0]) * jnp.sin(angles[1]), jnp.cos(angles[0])], 0)
    density_left, velocity_left, pressure_left = face_states(left_cells, offsets[0:3])
    density_right, velocity_right, pressure_right = face_states(right_cells, offsets[3:6])
    speed_left, energy_left, state_left, flux_left = conserved_flux(density_left, velocity_left, pressure_left, normal)
    speed_right, energy_right, state_right, flux_right = conserved_flux(density_right, velocity_right, pressure_right, normal)
    sound_left = jnp.sqrt(adiabatic * pressure_left / density_left)
    sound_right = jnp.sqrt(adiabatic * pressure_right / density_right)
    signal_left = jnp.minimum(speed_left - sound_left, speed_right - sound_right)
    signal_right = jnp.maximum(speed_left + sound_left, speed_right + sound_right)
    mass_left = density_left * (signal_left - speed_left)
    mass_right = density_right * (signal_right - speed_right)
    contact = (pressure_right - pressure_left + mass_left * speed_left - mass_right * speed_right) / (mass_left - mass_right)
    star_left = star_flux(density_left, velocity_left, pressure_left, normal, speed_left, energy_left, state_left, flux_left, signal_left, contact)
    star_right = star_flux(density_right, velocity_right, pressure_right, normal, speed_right, energy_right, state_right, flux_right, signal_right, contact)
    return jnp.where(signal_left >= 0, flux_left, jnp.where(contact >= 0, star_left, jnp.where(signal_right > 0, star_right, flux_right)))

def cell_conserved(primitive):
    density = jnp.exp(primitive[0])
    pressure = jnp.exp(primitive[4])
    velocity = primitive[1:4]
    energy = pressure / (adiabatic - 1.0) + 0.5 * density * lax.optimization_barrier(jnp.sum(velocity * velocity, axis=0))
    return jnp.concatenate([density[None], density * velocity, energy[None]], 0)

def signal_limit(primitive, volume):
    density = jnp.exp(primitive[0])
    pressure = jnp.exp(primitive[4])
    velocity = primitive[1:4]
    sound_speed = jnp.sqrt(adiabatic * pressure / density)
    flow_speed = jnp.sqrt(lax.optimization_barrier(jnp.sum(velocity * velocity, axis=0)))
    return volume ** (1.0 / 3.0) / (sound_speed + flow_speed)

def reference(primitive, gradient, volume, face_left, face_right, face_angles, face_area, face_offsets, rim_left, rim_right, rim_angles, rim_area, rim_offsets, send_list):
    devices = N_DOM * N_SUB
    local_cells = NB * BLK
    ghost_cells = N_SUB * CAP * BLK
    rim_width = RIM * BLK
    rim_faces = RIM * BLK
    packed = jnp.concatenate([primitive, gradient], 0)
    blocks = packed.reshape(20, devices * NB, BLK)
    wanted = send_list.reshape(N_DOM, N_SUB, N_SUB, CAP)
    owner = (jnp.arange(N_DOM, dtype=jnp.int32)[:, None, None, None] * N_SUB + jnp.arange(N_SUB, dtype=jnp.int32)[None, :, None, None]) * NB
    global_ids = jnp.transpose(owner + jnp.maximum(wanted, 0), (0, 2, 1, 3)).reshape(-1).astype(jnp.int32)
    in_use = jnp.transpose(wanted >= 0, (0, 2, 1, 3)).reshape(-1)
    ghosts = jnp.take(blocks, global_ids, axis=1) * in_use.astype(jnp.float32)[None, :, None]
    ghosts = ghosts.reshape(20, devices, ghost_cells)
    segments = packed.reshape(20, N_DOM, N_SUB, local_cells)
    following = jnp.concatenate([segments[:, 1:, :, :rim_width], jnp.zeros((20, 1, N_SUB, rim_width), jnp.float32)], 1).reshape(20, devices, rim_width)
    local_view = packed.reshape(20, devices, local_cells)

    def one_device(device):
        own_cells = lax.dynamic_index_in_dim(local_view, device, 1, keepdims=False)
        own_ghosts = lax.dynamic_index_in_dim(ghosts, device, 1, keepdims=False)
        next_cells = lax.dynamic_index_in_dim(following, device, 1, keepdims=False)
        left_index = lax.dynamic_slice_in_dim(face_left, device * FACES, FACES)
        right_index = lax.dynamic_slice_in_dim(face_right, device * FACES, FACES)
        angles = lax.dynamic_slice_in_dim(face_angles, device * FACES, FACES, 1)
        areas = lax.dynamic_slice_in_dim(face_area, device * FACES, FACES)
        offsets = lax.dynamic_slice_in_dim(face_offsets, device * FACES, FACES, 1)
        combined = jnp.concatenate([own_cells, own_ghosts], 1)
        weighted = hllc_flux(jnp.take(own_cells, left_index, axis=1), jnp.take(combined, right_index, axis=1), angles, offsets) * areas
        totals = jnp.zeros((5, local_cells + ghost_cells), jnp.float32).at[:, left_index].add(weighted).at[:, right_index].add(-weighted)
        rim_lidx = lax.dynamic_slice_in_dim(rim_left, device * rim_faces, rim_faces)
        rim_ridx = lax.dynamic_slice_in_dim(rim_right, device * rim_faces, rim_faces)
        rim_ang = lax.dynamic_slice_in_dim(rim_angles, device * rim_faces, rim_faces, 1)
        rim_areas = lax.dynamic_slice_in_dim(rim_area, device * rim_faces, rim_faces)
        rim_offs = lax.dynamic_slice_in_dim(rim_offsets, device * rim_faces, rim_faces, 1)
        rim_mask = (device // N_SUB < N_DOM - 1).astype(jnp.float32)
        tail_cells = own_cells[:, local_cells - rim_width:]
        rim_flux = hllc_flux(jnp.take(tail_cells, rim_lidx, axis=1), jnp.take(next_cells, rim_ridx, axis=1), rim_ang, rim_offs) * (rim_areas * rim_mask)
        net_flux = totals[:, :local_cells].at[:, local_cells - rim_width + rim_lidx].add(rim_flux)
        rim_back = jnp.zeros((5, rim_width), jnp.float32).at[:, rim_ridx].add(-rim_flux)
        return (net_flux, totals[:, local_cells:], rim_back)
    net_parts, ghost_back, rim_back = lax.map(one_device, jnp.arange(devices, dtype=jnp.int32))
    ghost_back = jnp.transpose(ghost_back, (1, 0, 2)).reshape(5, devices * N_SUB * CAP, BLK)
    target = jnp.where(in_use, global_ids, devices * NB).astype(jnp.int32)
    returned = jnp.zeros((5, devices * NB, BLK), jnp.float32).at[:, target].add(ghost_back, mode='drop')
    net_flux = jnp.transpose(net_parts, (1, 0, 2)) + returned.reshape(5, devices, local_cells)
    rim_inflow = jnp.concatenate([jnp.zeros((N_SUB, 5, rim_width), jnp.float32), rim_back[:devices - N_SUB]], 0)
    net_flux = net_flux.at[:, :, :rim_width].add(jnp.transpose(rim_inflow, (1, 0, 2)))
    net_flux = net_flux.reshape(5, devices * local_cells)
    time_step = courant * jnp.min(signal_limit(primitive, volume))
    change_rate = -net_flux / volume
    new_conserved = cell_conserved(primitive) + time_step * change_rate
    return (change_rate, new_conserved, time_step)
```

```python
import functools
import jax
import jax.numpy as jnp
from jax import lax
from jax.experimental import pallas as pl
from jax.experimental.pallas import tpu as pltpu
from jax.sharding import PartitionSpec as P

BLK = 128
RIM = 4
GROUP = 4
PIECES = 2

adiabatic = 5.0 / 3.0
courant = 0.3
MESH = pl.DeviceIdType.MESH


def side_state(q, offsets):
    def value(c):
        slopes = q(5 + 3 * c) * offsets[0] + q(6 + 3 * c) * offsets[1] + q(7 + 3 * c) * offsets[2]
        return q(c) + slopes

    return jnp.exp(value(0)), [value(1), value(2), value(3)], jnp.exp(value(4))


def conserved_flux(density, velocity, pressure, normal):
    speed = velocity[0] * normal[0] + velocity[1] * normal[1] + velocity[2] * normal[2]
    square = velocity[0] * velocity[0] + velocity[1] * velocity[1] + velocity[2] * velocity[2]
    energy = pressure / (adiabatic - 1.0) + 0.5 * density * square
    momentum = [density * v for v in velocity]
    conserved = [density] + momentum + [energy]
    flux = (
        [density * speed]
        + [m * speed + pressure * n for m, n in zip(momentum, normal)]
        + [(energy + pressure) * speed]
    )
    return speed, energy, conserved, flux


def star_flux(density, velocity, pressure, normal, speed, energy, conserved, flux, signal, contact, mass_rate):
    factor = mass_rate / (signal - contact)
    jump = contact - speed
    star = (
        [factor]
        + [factor * (v + jump * n) for v, n in zip(velocity, normal)]
        + [factor * (energy / density + jump * (contact + pressure / mass_rate))]
    )
    return [f + signal * (s - u) for f, s, u in zip(flux, star, conserved)]


def hllc(left, right, angles, offsets):
    sin_a = jnp.sin(angles[0])
    normal = [sin_a * jnp.cos(angles[1]), sin_a * jnp.sin(angles[1]), jnp.cos(angles[0])]
    dl, vl, pl_ = side_state(left, offsets[:3])
    dr, vr, pr = side_state(right, offsets[3:])
    ul, el, cl, fl = conserved_flux(dl, vl, pl_, normal)
    ur, er, cr, fr = conserved_flux(dr, vr, pr, normal)
    sound_l = jnp.sqrt(adiabatic * pl_ / dl)
    sound_r = jnp.sqrt(adiabatic * pr / dr)
    signal_l = jnp.minimum(ul - sound_l, ur - sound_r)
    signal_r = jnp.maximum(ul + sound_l, ur + sound_r)
    mass_l = dl * (signal_l - ul)
    mass_r = dr * (signal_r - ur)
    contact = (pr - pl_ + mass_l * ul - mass_r * ur) / (mass_l - mass_r)
    star_l = star_flux(dl, vl, pl_, normal, ul, el, cl, fl, signal_l, contact, mass_l)
    star_r = star_flux(dr, vr, pr, normal, ur, er, cr, fr, signal_r, contact, mass_r)
    out = []
    for a, b, c, d in zip(fl, star_l, star_r, fr):
        inner = jnp.where(contact >= 0, b, jnp.where(signal_r > 0, c, d))
        out.append(jnp.where(signal_l >= 0, a, inner))
    return out


def lane_gather(row, index):
    table = jnp.broadcast_to(row, index.shape)
    return jnp.take_along_axis(table, index, axis=1, mode="promise_in_bounds")


def kernel(
    dims,
    send_list,
    prim,
    grad,
    volume,
    face_left,
    face_right,
    face_angles,
    face_area,
    face_offsets,
    rim_left,
    rim_right,
    rim_angles,
    rim_area,
    rim_offsets,
    rate_out,
    new_out,
    step_out,
    outgoing,
    ghosts,
    following,
    table,
    min_own,
    min_sub,
    min_group,
    min_dom,
    gback_send,
    gback_recv,
    rback_send,
    rback_recv,
    cells,
    hi_left,
    lo_left,
    hi_right,
    lo_right,
    angles,
    offsets,
    area,
    gathered_l,
    gathered_r,
    pieces,
    ghost_send_sem,
    ghost_recv_sem,
    rim_send_sem,
    rim_recv_sem,
    min_send_sem,
    min_recv_sem,
    dmin_send_sem,
    dmin_recv_sem,
    gback_send_sem,
    gback_recv_sem,
    rback_send_sem,
    rback_recv_sem,
):
    n_dom, n_sub, capacity, blocks, face_rows = dims
    rows = face_rows + RIM
    ghost_blocks = n_sub * capacity
    me_dom = lax.axis_index("dom")
    me_sub = lax.axis_index("sub")
    before = lax.rem(me_dom + n_dom - 1, n_dom)
    after = lax.rem(me_dom + 1, n_dom)

    def sub_peer(off):
        return lax.rem(me_sub + off, n_sub)

    def dom_peer(off):
        return lax.rem(me_dom + off, n_dom)

    barrier = pltpu.get_barrier_semaphore()
    for off in range(1, n_sub):
        pl.semaphore_signal(barrier, inc=1, device_id=(me_dom, sub_peer(off)), device_id_type=MESH)
    for off in range(1, n_dom):
        pl.semaphore_signal(barrier, inc=1, device_id=(dom_peer(off), me_sub), device_id_type=MESH)

    for h in range(blocks):
        table[h, 0:5, :] = prim[:, h * BLK : (h + 1) * BLK]
        table[h, 5:8, :] = jnp.zeros((3, BLK), jnp.float32)
        table[h, 8:23, :] = grad[:, h * BLK : (h + 1) * BLK]
        table[h, 23:24, :] = jnp.zeros((1, BLK), jnp.float32)

    for off in range(1, n_sub):
        for j in range(capacity):
            block = jnp.maximum(send_list[sub_peer(off) * capacity + j], 0)
            outgoing[off, j] = table[block]

    for r in range(5):
        for h in range(blocks):
            cells[r, h : h + 1, :] = prim[r : r + 1, h * BLK : (h + 1) * BLK]
    density = jnp.exp(cells[0])
    pressure = jnp.exp(cells[4])
    square = cells[1] * cells[1] + cells[2] * cells[2] + cells[3] * cells[3]
    signal = jnp.sqrt(adiabatic * pressure / density) + jnp.sqrt(square)
    limit = jnp.exp(jnp.log(volume[...]) * (1.0 / 3.0)) / signal
    local_min = jnp.min(limit)
    min_own[...] = jnp.full(min_own.shape, local_min, jnp.float32)

    pl.semaphore_wait(barrier, n_sub - 1 + n_dom - 1)

    copies = []

    def ghost_copy(off):
        return pltpu.make_async_remote_copy(
            src_ref=outgoing.at[off],
            dst_ref=ghosts.at[off],
            send_sem=ghost_send_sem.at[off],
            recv_sem=ghost_recv_sem.at[off],
            device_id=(me_dom, sub_peer(off)),
            device_id_type=MESH,
        )

    ghost_copies = [ghost_copy(off) for off in range(1, n_sub)]
    for copy in ghost_copies:
        copy.start()
    rim_copy = pltpu.make_async_remote_copy(
        src_ref=table.at[0:RIM],
        dst_ref=following,
        send_sem=rim_send_sem,
        recv_sem=rim_recv_sem,
        device_id=(before, me_sub),
        device_id_type=MESH,
    )
    rim_copy.start()
    min_copies = [
        pltpu.make_async_remote_copy(
            src_ref=min_own,
            dst_ref=min_sub.at[off],
            send_sem=min_send_sem.at[off],
            recv_sem=min_recv_sem.at[off],
            device_id=(me_dom, sub_peer(off)),
            device_id_type=MESH,
        )
        for off in range(1, n_sub)
    ]
    for copy in min_copies:
        copy.start()

    hi_left[0:face_rows, :] = face_left[...] // BLK
    lo_left[0:face_rows, :] = lax.rem(face_left[...], BLK)
    hi_right[0:face_rows, :] = face_right[...] // BLK
    lo_right[0:face_rows, :] = lax.rem(face_right[...], BLK)
    area[0:face_rows, :] = face_area[...]
    twice = lambda ref: jnp.concatenate([ref[...], ref[...]], 0)
    hi_left[face_rows : face_rows + 8, :] = twice(rim_left) // BLK + (blocks - RIM)
    lo_left[face_rows : face_rows + 8, :] = lax.rem(twice(rim_left), BLK)
    hi_right[face_rows : face_rows + 8, :] = twice(rim_right) // BLK + (blocks + ghost_blocks)
    lo_right[face_rows : face_rows + 8, :] = lax.rem(twice(rim_right), BLK)
    last = me_dom == n_dom - 1
    area[face_rows : face_rows + 8, :] = twice(rim_area)
    for s in range(face_rows):
        for r in range(2):
            angles[r, s : s + 1, :] = face_angles[r : r + 1, s * BLK : (s + 1) * BLK]
        for r in range(6):
            offsets[r, s : s + 1, :] = face_offsets[r : r + 1, s * BLK : (s + 1) * BLK]
    for s in range(8):
        t = s % RIM
        for r in range(2):
            angles[r, face_rows + s : face_rows + s + 1, :] = rim_angles[r : r + 1, t * BLK : (t + 1) * BLK]
        for r in range(6):
            offsets[r, face_rows + s : face_rows + s + 1, :] = rim_offsets[r : r + 1, t * BLK : (t + 1) * BLK]

    main = pl.ds(0, face_rows)
    tail = pl.ds(face_rows, 8)

    def gather_local(count, place, shift):
        def step(r, carry):
            hl, ll, hr, lr = (ref[main, :] for ref in (hi_left, lo_left, hi_right, lo_right))
            left = jnp.zeros(hl.shape, jnp.float32)
            right = jnp.zeros(hl.shape, jnp.float32)
            for h in range(blocks):
                row = table[h, pl.ds(r + place, 1), :]
                left = jnp.where(hl == h, lane_gather(row, ll), left)
                right = jnp.where(hr == h, lane_gather(row, lr), right)
            gathered_l[r + shift, main, :] = left
            gathered_r[r + shift, main, :] = right
            hl, ll = hi_left[tail, :], lo_left[tail, :]
            left = jnp.zeros(hl.shape, jnp.float32)
            for h in range(blocks - RIM, blocks):
                row = table[h, pl.ds(r + place, 1), :]
                left = jnp.where(hl == h, lane_gather(row, ll), left)
            gathered_l[r + shift, tail, :] = left
            return carry

        lax.fori_loop(0, count, step, 0)

    gather_local(5, 0, 0)
    gather_local(15, 8, 5)

    for copy in min_copies:
        copy.wait()
    group_min = min_own[...]
    for off in range(1, n_sub):
        group_min = jnp.minimum(group_min, min_sub[off])
    min_group[...] = group_min

    rim_copy.wait()

    def gather_rim(count, place, shift):
        def step(r, carry):
            hr, lr = hi_right[tail, :], lo_right[tail, :]
            right = jnp.zeros(hr.shape, jnp.float32)
            for h in range(RIM):
                row = following[h, pl.ds(r + place, 1), :]
                right = jnp.where(hr == h + blocks + ghost_blocks, lane_gather(row, lr), right)
            gathered_r[r + shift, tail, :] = right
            return carry

        lax.fori_loop(0, count, step, 0)

    gather_rim(5, 0, 0)
    gather_rim(15, 8, 5)

    dmin_copies = [
        pltpu.make_async_remote_copy(
            src_ref=min_group,
            dst_ref=min_dom.at[off],
            send_sem=dmin_send_sem.at[off],
            recv_sem=dmin_recv_sem.at[off],
            device_id=(dom_peer(off), me_sub),
            device_id_type=MESH,
        )
        for off in range(1, n_dom)
    ]
    for copy in dmin_copies:
        copy.start()

    for copy in ghost_copies:
        copy.wait()

    def gather_ghosts(count, place, shift):
        def step(r, carry):
            hr, lr = hi_right[main, :], lo_right[main, :]
            right = gathered_r[r + shift, main, :]
            for off in range(1, n_sub):
                sender = lax.rem(me_sub + n_sub - off, n_sub)
                for j in range(capacity):
                    row = ghosts[off, j, pl.ds(r + place, 1), :]
                    right = jnp.where(hr == blocks + sender * capacity + j, lane_gather(row, lr), right)
            gathered_r[r + shift, main, :] = right
            return carry

        lax.fori_loop(0, count, step, 0)

    gather_ghosts(5, 0, 0)
    gather_ghosts(15, 8, 5)

    def flux_step(g, carry):
        here = pl.ds(pl.multiple_of(g * 8, 8), 8)
        flux = hllc(
            lambda c: gathered_l[c, here, :],
            lambda c: gathered_r[c, here, :],
            [angles[k, here, :] for k in range(2)],
            [offsets[k, here, :] for k in range(6)],
        )
        idle = jnp.logical_and(g * 8 >= face_rows, last)
        for c in range(5):
            value = jnp.where(idle, 0.0, flux[c] * area[here, :])
            big = value.astype(jnp.bfloat16).astype(jnp.float32)
            pieces[c, here, :] = big
            pieces[5 + c, here, :] = value - big
        return carry

    lax.fori_loop(0, (face_rows + 8) // 8, flux_step, 0)

    lane_iota = lax.broadcasted_iota(jnp.int32, (BLK, BLK), 0)

    def one_hot(lo, s):
        return jnp.where(lane_iota == lo[pl.ds(s, 1), :], 1.0, 0.0).astype(jnp.bfloat16)

    def spread(hi, s, first, count, sign):
        place = lax.broadcasted_iota(jnp.int32, (count, BLK), 0) + first
        match = place == hi[pl.ds(s, 1), :]
        parts = []
        for c in range(5 * PIECES):
            value = pieces[c, pl.ds(s, 1), :]
            value = value if sign > 0 else -value
            parts.append(jnp.where(match, value, 0.0))
        return jnp.concatenate(parts, 0).astype(jnp.bfloat16)

    def product(a, b):
        return lax.dot_general(a, b, (((1,), (1,)), ((), ())), preferred_element_type=jnp.float32)

    def fold(total, count):
        total = total.reshape(PIECES, 5, count, BLK)
        return total[0] + total[1]

    away = -(-(ghost_blocks + RIM) // 8) * 8

    def away_step(i, total):
        a = jnp.concatenate([spread(hi_right, i * GROUP + k, blocks, away, -1) for k in range(GROUP)], 1)
        b = jnp.concatenate([one_hot(lo_right, i * GROUP + k) for k in range(GROUP)], 1)
        return total + product(a, b)

    total = lax.fori_loop(0, rows // GROUP, away_step, jnp.zeros((5 * PIECES * away, BLK), jnp.float32))
    total = fold(total, away)
    for s in range(n_sub):
        gback_send[s] = total[:, s * capacity : (s + 1) * capacity, :]
    rback_send[...] = total[:, ghost_blocks : ghost_blocks + RIM, :]
    gback_copies = [
        pltpu.make_async_remote_copy(
            src_ref=gback_send.at[sub_peer(off)],
            dst_ref=gback_recv.at[off],
            send_sem=gback_send_sem.at[off],
            recv_sem=gback_recv_sem.at[off],
            device_id=(me_dom, sub_peer(off)),
            device_id_type=MESH,
        )
        for off in range(1, n_sub)
    ]
    for copy in gback_copies:
        copy.start()
    rback_copy = pltpu.make_async_remote_copy(
        src_ref=rback_send,
        dst_ref=rback_recv,
        send_sem=rback_send_sem,
        recv_sem=rback_recv_sem,
        device_id=(after, me_sub),
        device_id_type=MESH,
    )
    rback_copy.start()

    def local_step(i, total):
        a = [spread(hi_left, i * GROUP + k, 0, blocks, 1) for k in range(GROUP)]
        a += [spread(hi_right, i * GROUP + k, 0, blocks, -1) for k in range(GROUP)]
        b = [one_hot(lo_left, i * GROUP + k) for k in range(GROUP)]
        b += [one_hot(lo_right, i * GROUP + k) for k in range(GROUP)]
        return total + product(jnp.concatenate(a, 1), jnp.concatenate(b, 1))

    total = lax.fori_loop(0, rows // GROUP, local_step, jnp.zeros((5 * PIECES * blocks, BLK), jnp.float32))
    net = fold(total, blocks)

    for copy in dmin_copies:
        copy.wait()
    smallest = min_group[...]
    for off in range(1, n_dom):
        smallest = jnp.minimum(smallest, min_dom[off])
    time_step = courant * smallest
    step_out[...] = time_step
    time_step = time_step[0:1, :]

    rback_copy.wait()
    for copy in gback_copies:
        copy.wait()

    place = lax.broadcasted_iota(jnp.int32, (blocks, BLK), 0)
    density = jnp.exp(cells[0])
    pressure = jnp.exp(cells[4])
    square = cells[1] * cells[1] + cells[2] * cells[2] + cells[3] * cells[3]
    energy = pressure / (adiabatic - 1.0) + 0.5 * density * square
    conserved = [density, density * cells[1], density * cells[2], density * cells[3], energy]
    for c in range(5):
        sums = net[c]
        for h in range(RIM):
            sums = sums + jnp.where(place == h, rback_recv[c, h : h + 1, :], 0.0)
        for off in range(1, n_sub):
            sender = lax.rem(me_sub + n_sub - off, n_sub)
            for j in range(capacity):
                wanted = send_list[sender * capacity + j]
                sums = sums + jnp.where(place == wanted, gback_recv[off, c, j : j + 1, :], 0.0)
        rate = -sums / volume[...]
        rate_out[c] = rate
        new_out[c] = conserved[c] + time_step * rate


def body(mesh_sizes, *args):
    (primitive, gradient, volume, face_left, face_right, face_angles, face_area, face_offsets) = args[:8]
    (rim_left, rim_right, rim_angles, rim_area, rim_offsets, send_list) = args[8:]
    n_dom, n_sub = mesh_sizes
    cells = primitive.shape[1]
    blocks = cells // BLK
    face_rows = face_left.shape[0] // BLK
    capacity = send_list.shape[0] // n_sub
    padded = face_rows + 8
    dims = (n_dom, n_sub, capacity, blocks, face_rows)
    f32, i32 = jnp.float32, jnp.int32
    vmem = pl.BlockSpec(memory_space=pltpu.VMEM)
    smem = pl.BlockSpec(memory_space=pltpu.SMEM)
    sem = pltpu.SemaphoreType.DMA
    rate, new, step = pl.pallas_call(
        functools.partial(kernel, dims),
        out_shape=(
            jax.ShapeDtypeStruct((5, blocks, BLK), f32),
            jax.ShapeDtypeStruct((5, blocks, BLK), f32),
            jax.ShapeDtypeStruct((8, BLK), f32),
        ),
        in_specs=[smem] + [vmem] * 13,
        out_specs=(vmem, vmem, vmem),
        scratch_shapes=[
            pltpu.VMEM((n_sub, capacity, 24, BLK), f32),
            pltpu.VMEM((n_sub, capacity, 24, BLK), f32),
            pltpu.VMEM((RIM, 24, BLK), f32),
            pltpu.VMEM((blocks, 24, BLK), f32),
            pltpu.VMEM((8, BLK), f32),
            pltpu.VMEM((n_sub, 8, BLK), f32),
            pltpu.VMEM((8, BLK), f32),
            pltpu.VMEM((n_dom, 8, BLK), f32),
            pltpu.VMEM((n_sub, 5, capacity, BLK), f32),
            pltpu.VMEM((n_sub, 5, capacity, BLK), f32),
            pltpu.VMEM((5, RIM, BLK), f32),
            pltpu.VMEM((5, RIM, BLK), f32),
            pltpu.VMEM((5, blocks, BLK), f32),
            pltpu.VMEM((padded, BLK), i32),
            pltpu.VMEM((padded, BLK), i32),
            pltpu.VMEM((padded, BLK), i32),
            pltpu.VMEM((padded, BLK), i32),
            pltpu.VMEM((2, padded, BLK), f32),
            pltpu.VMEM((6, padded, BLK), f32),
            pltpu.VMEM((padded, BLK), f32),
            pltpu.VMEM((20, padded, BLK), f32),
            pltpu.VMEM((20, padded, BLK), f32),
            pltpu.VMEM((5 * PIECES, padded, BLK), f32),
            sem((n_sub,)),
            sem((n_sub,)),
            sem,
            sem,
            sem((n_sub,)),
            sem((n_sub,)),
            sem((n_dom,)),
            sem((n_dom,)),
            sem((n_sub,)),
            sem((n_sub,)),
            sem,
            sem,
        ],
        compiler_params=pltpu.CompilerParams(collective_id=0, has_side_effects=True),
        name="hydro_step",
    )(
        send_list,
        primitive,
        gradient,
        volume.reshape(blocks, BLK),
        face_left.reshape(face_rows, BLK),
        face_right.reshape(face_rows, BLK),
        face_angles,
        face_area.reshape(face_rows, BLK),
        face_offsets,
        rim_left.reshape(RIM, BLK),
        rim_right.reshape(RIM, BLK),
        rim_angles,
        rim_area.reshape(RIM, BLK),
        rim_offsets,
    )
    return rate.reshape(5, cells), new.reshape(5, cells), step[0, 0]


def solution(mesh):
    both = ("dom", "sub")
    wide, flat = P(None, both), P(both)
    in_specs = (wide, wide, flat, flat, flat, wide, flat, wide, flat, flat, wide, flat, wide, flat)
    out_specs = (wide, wide, P())
    step = functools.partial(body, (mesh.shape["dom"], mesh.shape["sub"]))
    return jax.shard_map(step, mesh=mesh, in_specs=in_specs, out_specs=out_specs, check_vma=False)
```

```python
import functools
import jax
import jax.numpy as jnp
from jax import lax
from jax.experimental import pallas as pl
from jax.experimental.pallas import tpu as pltpu
from jax.sharding import PartitionSpec as P

BLK = 128
RIM = 4
GROUP = 13
PIECES = 2

adiabatic = 5.0 / 3.0
courant = 0.3
MESH = pl.DeviceIdType.MESH


def side_state(q, offsets):
    def value(c):
        slopes = q(5 + 3 * c) * offsets[0] + q(6 + 3 * c) * offsets[1] + q(7 + 3 * c) * offsets[2]
        return q(c) + slopes

    return jnp.exp(value(0)), [value(1), value(2), value(3)], jnp.exp(value(4))


def conserved_flux(density, velocity, pressure, normal):
    speed = velocity[0] * normal[0] + velocity[1] * normal[1] + velocity[2] * normal[2]
    square = velocity[0] * velocity[0] + velocity[1] * velocity[1] + velocity[2] * velocity[2]
    energy = pressure / (adiabatic - 1.0) + 0.5 * density * square
    momentum = [density * v for v in velocity]
    conserved = [density] + momentum + [energy]
    flux = (
        [density * speed]
        + [m * speed + pressure * n for m, n in zip(momentum, normal)]
        + [(energy + pressure) * speed]
    )
    return speed, energy, conserved, flux


def star_flux(density, velocity, pressure, normal, speed, energy, conserved, flux, signal, contact, mass_rate):
    factor = mass_rate / (signal - contact)
    jump = contact - speed
    star = (
        [factor]
        + [factor * (v + jump * n) for v, n in zip(velocity, normal)]
        + [factor * (energy / density + jump * (contact + pressure / mass_rate))]
    )
    return [f + signal * (s - u) for f, s, u in zip(flux, star, conserved)]


def hllc(left, right, angles, offsets):
    sin_a = jnp.sin(angles[0])
    normal = [sin_a * jnp.cos(angles[1]), sin_a * jnp.sin(angles[1]), jnp.cos(angles[0])]
    dl, vl, pl_ = side_state(left, offsets[:3])
    dr, vr, pr = side_state(right, offsets[3:])
    ul, el, cl, fl = conserved_flux(dl, vl, pl_, normal)
    ur, er, cr, fr = conserved_flux(dr, vr, pr, normal)
    sound_l = jnp.sqrt(adiabatic * pl_ / dl)
    sound_r = jnp.sqrt(adiabatic * pr / dr)
    signal_l = jnp.minimum(ul - sound_l, ur - sound_r)
    signal_r = jnp.maximum(ul + sound_l, ur + sound_r)
    mass_l = dl * (signal_l - ul)
    mass_r = dr * (signal_r - ur)
    contact = (pr - pl_ + mass_l * ul - mass_r * ur) / (mass_l - mass_r)
    star_l = star_flux(dl, vl, pl_, normal, ul, el, cl, fl, signal_l, contact, mass_l)
    star_r = star_flux(dr, vr, pr, normal, ur, er, cr, fr, signal_r, contact, mass_r)
    out = []
    for a, b, c, d in zip(fl, star_l, star_r, fr):
        inner = jnp.where(contact >= 0, b, jnp.where(signal_r > 0, c, d))
        out.append(jnp.where(signal_l >= 0, a, inner))
    return out


def lane_gather(row, index):
    table = jnp.broadcast_to(row, index.shape)
    return jnp.take_along_axis(table, index, axis=1, mode="promise_in_bounds")


def kernel(dims, send_list, *refs):
    staged = refs[16:29]
    stage_sem = refs[29]
    loads = [pltpu.make_async_copy(source, staged[k], stage_sem.at[k]) for k, source in enumerate(refs[:13])]
    step(dims, send_list, loads, *staged, *refs[13:16], *refs[30:])


def step(
    dims,
    send_list,
    loads,
    prim,
    grad,
    volume,
    face_left,
    face_right,
    face_angles,
    face_area,
    face_offsets,
    rim_left,
    rim_right,
    rim_angles,
    rim_area,
    rim_offsets,
    rate_out,
    new_out,
    step_out,
    outgoing,
    ghosts,
    following,
    table,
    min_own,
    min_sub,
    min_group,
    min_dom,
    gback_send,
    gback_recv,
    rback_send,
    rback_recv,
    cells,
    hi_left,
    lo_left,
    hi_right,
    lo_right,
    angles,
    offsets,
    area,
    gathered_l,
    gathered_r,
    pieces,
    ghost_send_sem,
    ghost_recv_sem,
    rim_send_sem,
    rim_recv_sem,
    min_send_sem,
    min_recv_sem,
    dmin_send_sem,
    dmin_recv_sem,
    gback_send_sem,
    gback_recv_sem,
    rback_send_sem,
    rback_recv_sem,
):
    n_dom, n_sub, capacity, blocks, face_rows = dims
    rows = face_rows + RIM
    group = max(k for k in range(1, GROUP + 1) if rows % k == 0)
    ghost_blocks = n_sub * capacity
    me_dom = lax.axis_index("dom")
    me_sub = lax.axis_index("sub")
    before = lax.rem(me_dom + n_dom - 1, n_dom)
    after = lax.rem(me_dom + 1, n_dom)

    def sub_peer(off):
        return lax.rem(me_sub + off, n_sub)

    def dom_peer(off):
        return lax.rem(me_dom + off, n_dom)

    barrier = pltpu.get_barrier_semaphore()
    for off in range(1, n_sub):
        pl.semaphore_signal(barrier, inc=1, device_id=(me_dom, sub_peer(off)), device_id_type=MESH)
    for off in range(1, n_dom):
        pl.semaphore_signal(barrier, inc=1, device_id=(dom_peer(off), me_sub), device_id_type=MESH)

    for load in loads:
        load.start()
    for k in (0, 1):
        loads[k].wait()

    for h in range(blocks):
        table[h, 0:5, :] = prim[:, h * BLK : (h + 1) * BLK]
        table[h, 5:8, :] = jnp.zeros((3, BLK), jnp.float32)
        table[h, 8:23, :] = grad[:, h * BLK : (h + 1) * BLK]
        table[h, 23:24, :] = jnp.zeros((1, BLK), jnp.float32)

    for off in range(1, n_sub):
        for j in range(capacity):
            block = jnp.maximum(send_list[sub_peer(off) * capacity + j], 0)
            outgoing[off, j] = table[block]

    for k in range(2, len(loads)):
        loads[k].wait()

    for r in range(5):
        for h in range(blocks):
            cells[r, h : h + 1, :] = prim[r : r + 1, h * BLK : (h + 1) * BLK]
    density = jnp.exp(cells[0])
    pressure = jnp.exp(cells[4])
    square = cells[1] * cells[1] + cells[2] * cells[2] + cells[3] * cells[3]
    signal = jnp.sqrt(adiabatic * pressure / density) + jnp.sqrt(square)
    limit = jnp.exp(jnp.log(volume[...]) * (1.0 / 3.0)) / signal
    local_min = jnp.min(limit)
    min_own[...] = jnp.full(min_own.shape, local_min, jnp.float32)

    hi_left[0:face_rows, :] = face_left[...] // BLK
    lo_left[0:face_rows, :] = lax.rem(face_left[...], BLK)
    hi_right[0:face_rows, :] = face_right[...] // BLK
    lo_right[0:face_rows, :] = lax.rem(face_right[...], BLK)
    area[0:face_rows, :] = face_area[...]
    twice = lambda ref: jnp.concatenate([ref[...], ref[...]], 0)
    hi_left[face_rows : face_rows + 8, :] = twice(rim_left) // BLK + (blocks - RIM)
    lo_left[face_rows : face_rows + 8, :] = lax.rem(twice(rim_left), BLK)
    hi_right[face_rows : face_rows + 8, :] = twice(rim_right) // BLK + (blocks + ghost_blocks)
    lo_right[face_rows : face_rows + 8, :] = lax.rem(twice(rim_right), BLK)
    last = me_dom == n_dom - 1
    area[face_rows : face_rows + 8, :] = twice(rim_area)
    for s in range(face_rows):
        for r in range(2):
            angles[r, s : s + 1, :] = face_angles[r : r + 1, s * BLK : (s + 1) * BLK]
        for r in range(6):
            offsets[r, s : s + 1, :] = face_offsets[r : r + 1, s * BLK : (s + 1) * BLK]
    for s in range(8):
        t = s % RIM
        for r in range(2):
            angles[r, face_rows + s : face_rows + s + 1, :] = rim_angles[r : r + 1, t * BLK : (t + 1) * BLK]
        for r in range(6):
            offsets[r, face_rows + s : face_rows + s + 1, :] = rim_offsets[r : r + 1, t * BLK : (t + 1) * BLK]

    tail = pl.ds(face_rows, 8)

    fields = list(range(5)) + list(range(8, 23))

    def gather(hi, lo, entries, names, start):
        match = [hi == name for name in names]
        out = []
        for c, place in enumerate(fields):
            value = start(c)
            for entry, hit in zip(entries, match):
                row = entry[place : place + 1, :]
                value = jnp.where(hit, lane_gather(row, lo), value)
            out.append(value)
        return out

    def gather_into(target, hi, lo, here, entries, names, keep):
        start = (lambda c: target[c, here, :]) if keep else (lambda c: jnp.zeros((8, BLK), jnp.float32))
        for c, value in enumerate(gather(hi[here, :], lo[here, :], entries, names, start)):
            target[c, here, :] = value

    def gather_main(target, hi, lo, entries, names, keep):
        def one(g, carry):
            here = pl.ds(pl.multiple_of(g * 8, 8), 8)
            gather_into(target, hi, lo, here, entries, names, keep)
            return carry

        lax.fori_loop(0, face_rows // 8, one, 0)

    own = [table.at[h] for h in range(blocks)]
    gather_main(gathered_l, hi_left, lo_left, own, range(blocks), False)

    pl.semaphore_wait(barrier, n_sub - 1 + n_dom - 1)

    copies = []

    def ghost_copy(off):
        return pltpu.make_async_remote_copy(
            src_ref=outgoing.at[off],
            dst_ref=ghosts.at[off],
            send_sem=ghost_send_sem.at[off],
            recv_sem=ghost_recv_sem.at[off],
            device_id=(me_dom, sub_peer(off)),
            device_id_type=MESH,
        )

    ghost_copies = [ghost_copy(off) for off in range(1, n_sub)]
    for copy in ghost_copies:
        copy.start()
    rim_copy = pltpu.make_async_remote_copy(
        src_ref=table.at[0:RIM],
        dst_ref=following,
        send_sem=rim_send_sem,
        recv_sem=rim_recv_sem,
        device_id=(before, me_sub),
        device_id_type=MESH,
    )
    rim_copy.start()
    min_copies = [
        pltpu.make_async_remote_copy(
            src_ref=min_own,
            dst_ref=min_sub.at[off],
            send_sem=min_send_sem.at[off],
            recv_sem=min_recv_sem.at[off],
            device_id=(me_dom, sub_peer(off)),
            device_id_type=MESH,
        )
        for off in range(1, n_sub)
    ]
    for copy in min_copies:
        copy.start()

    gather_into(gathered_l, hi_left, lo_left, tail, own[blocks - RIM :], range(blocks - RIM, blocks), False)
    gather_main(gathered_r, hi_right, lo_right, own, range(blocks), False)

    for copy in min_copies:
        copy.wait()
    group_min = min_own[...]
    for off in range(1, n_sub):
        group_min = jnp.minimum(group_min, min_sub[off])
    min_group[...] = group_min

    rim_copy.wait()

    first = blocks + ghost_blocks
    nexts = [following.at[h] for h in range(RIM)]
    gather_into(gathered_r, hi_right, lo_right, tail, nexts, range(first, first + RIM), False)

    dmin_copies = [
        pltpu.make_async_remote_copy(
            src_ref=min_group,
            dst_ref=min_dom.at[off],
            send_sem=dmin_send_sem.at[off],
            recv_sem=dmin_recv_sem.at[off],
            device_id=(dom_peer(off), me_sub),
            device_id_type=MESH,
        )
        for off in range(1, n_dom)
    ]
    for copy in dmin_copies:
        copy.start()

    for copy in ghost_copies:
        copy.wait()

    entries, names = [], []
    for off in range(1, n_sub):
        sender = lax.rem(me_sub + n_sub - off, n_sub)
        for j in range(capacity):
            entries.append(ghosts.at[off, j])
            names.append(blocks + sender * capacity + j)
    gather_main(gathered_r, hi_right, lo_right, entries, names, True)

    def flux_step(g, carry):
        here = pl.ds(pl.multiple_of(g * 8, 8), 8)
        flux = hllc(
            lambda c: gathered_l[c, here, :],
            lambda c: gathered_r[c, here, :],
            [angles[k, here, :] for k in range(2)],
            [offsets[k, here, :] for k in range(6)],
        )
        idle = jnp.logical_and(g * 8 >= face_rows, last)
        for c in range(5):
            value = jnp.where(idle, 0.0, flux[c] * area[here, :])
            big = value.astype(jnp.bfloat16).astype(jnp.float32)
            pieces[c, here, :] = big
            pieces[5 + c, here, :] = value - big
        return carry

    lax.fori_loop(0, (face_rows + 8) // 8, flux_step, 0)

    lane_iota = lax.broadcasted_iota(jnp.int32, (BLK, BLK), 0)

    def one_hot(lo, s):
        return jnp.where(lane_iota == lo[pl.ds(s, 1), :], 1.0, 0.0).astype(jnp.bfloat16)

    def spread(hi, s, first, count, sign):
        place = lax.broadcasted_iota(jnp.int32, (count, BLK), 0) + first
        match = place == hi[pl.ds(s, 1), :]
        parts = []
        for c in range(5 * PIECES):
            value = pieces[c, pl.ds(s, 1), :]
            value = value if sign > 0 else -value
            parts.append(jnp.where(match, value, 0.0))
        return jnp.concatenate(parts, 0).astype(jnp.bfloat16)

    def product(a, b):
        return lax.dot_general(a, b, (((1,), (1,)), ((), ())), preferred_element_type=jnp.float32)

    def fold(total, count):
        total = total.reshape(PIECES, 5, count, BLK)
        return total[0] + total[1]

    away = -(-(ghost_blocks + RIM) // 8) * 8

    def away_step(i, total):
        a = jnp.concatenate([spread(hi_right, i * group + k, blocks, away, -1) for k in range(group)], 1)
        b = jnp.concatenate([one_hot(lo_right, i * group + k) for k in range(group)], 1)
        return total + product(a, b)

    total = lax.fori_loop(0, rows // group, away_step, jnp.zeros((5 * PIECES * away, BLK), jnp.float32))
    total = fold(total, away)
    for s in range(n_sub):
        gback_send[s] = total[:, s * capacity : (s + 1) * capacity, :]
    rback_send[...] = total[:, ghost_blocks : ghost_blocks + RIM, :]
    gback_copies = [
        pltpu.make_async_remote_copy(
            src_ref=gback_send.at[sub_peer(off)],
            dst_ref=gback_recv.at[off],
            send_sem=gback_send_sem.at[off],
            recv_sem=gback_recv_sem.at[off],
            device_id=(me_dom, sub_peer(off)),
            device_id_type=MESH,
        )
        for off in range(1, n_sub)
    ]
    for copy in gback_copies:
        copy.start()
    rback_copy = pltpu.make_async_remote_copy(
        src_ref=rback_send,
        dst_ref=rback_recv,
        send_sem=rback_send_sem,
        recv_sem=rback_recv_sem,
        device_id=(after, me_sub),
        device_id_type=MESH,
    )
    rback_copy.start()

    def local_step(i, total):
        a = [spread(hi_left, i * group + k, 0, blocks, 1) for k in range(group)]
        a += [spread(hi_right, i * group + k, 0, blocks, -1) for k in range(group)]
        b = [one_hot(lo_left, i * group + k) for k in range(group)]
        b += [one_hot(lo_right, i * group + k) for k in range(group)]
        return total + product(jnp.concatenate(a, 1), jnp.concatenate(b, 1))

    total = lax.fori_loop(0, rows // group, local_step, jnp.zeros((5 * PIECES * blocks, BLK), jnp.float32))
    net = fold(total, blocks)

    for copy in dmin_copies:
        copy.wait()
    smallest = min_group[...]
    for off in range(1, n_dom):
        smallest = jnp.minimum(smallest, min_dom[off])
    time_step = courant * smallest
    step_out[0] = jnp.min(time_step)
    time_step = time_step[0:1, :]

    rback_copy.wait()
    for copy in gback_copies:
        copy.wait()

    place = lax.broadcasted_iota(jnp.int32, (blocks, BLK), 0)
    density = jnp.exp(cells[0])
    pressure = jnp.exp(cells[4])
    square = cells[1] * cells[1] + cells[2] * cells[2] + cells[3] * cells[3]
    energy = pressure / (adiabatic - 1.0) + 0.5 * density * square
    conserved = [density, density * cells[1], density * cells[2], density * cells[3], energy]
    for c in range(5):
        sums = net[c]
        for h in range(RIM):
            sums = sums + jnp.where(place == h, rback_recv[c, h : h + 1, :], 0.0)
        for off in range(1, n_sub):
            sender = lax.rem(me_sub + n_sub - off, n_sub)
            for j in range(capacity):
                wanted = send_list[sender * capacity + j]
                sums = sums + jnp.where(place == wanted, gback_recv[off, c, j : j + 1, :], 0.0)
        rate = -sums / volume[...]
        rate_out[c] = rate
        new_out[c] = conserved[c] + time_step * rate


def body(mesh_sizes, *args):
    (primitive, gradient, volume, face_left, face_right, face_angles, face_area, face_offsets) = args[:8]
    (rim_left, rim_right, rim_angles, rim_area, rim_offsets, send_list) = args[8:]
    n_dom, n_sub = mesh_sizes
    cells = primitive.shape[1]
    blocks = cells // BLK
    face_rows = face_left.shape[0] // BLK
    capacity = send_list.shape[0] // n_sub
    padded = face_rows + 8
    dims = (n_dom, n_sub, capacity, blocks, face_rows)
    f32, i32 = jnp.float32, jnp.int32
    vmem = pl.BlockSpec(memory_space=pltpu.VMEM)
    smem = pl.BlockSpec(memory_space=pltpu.SMEM)
    sem = pltpu.SemaphoreType.DMA
    operands = (
        primitive,
        gradient,
        volume.reshape(blocks, BLK),
        face_left.reshape(face_rows, BLK),
        face_right.reshape(face_rows, BLK),
        face_angles,
        face_area.reshape(face_rows, BLK),
        face_offsets,
        rim_left.reshape(RIM, BLK),
        rim_right.reshape(RIM, BLK),
        rim_angles,
        rim_area.reshape(RIM, BLK),
        rim_offsets,
    )
    rate, new, step = pl.pallas_call(
        functools.partial(kernel, dims),
        out_shape=(
            jax.ShapeDtypeStruct((5, blocks, BLK), f32),
            jax.ShapeDtypeStruct((5, blocks, BLK), f32),
            jax.ShapeDtypeStruct((1,), f32),
        ),
        in_specs=[smem] + [pl.BlockSpec(memory_space=pl.ANY)] * 13,
        out_specs=(vmem, vmem, smem),
        scratch_shapes=[pltpu.VMEM(x.shape, x.dtype) for x in operands]
        + [
            sem((len(operands),)),
            pltpu.VMEM((n_sub, capacity, 24, BLK), f32),
            pltpu.VMEM((n_sub, capacity, 24, BLK), f32),
            pltpu.VMEM((RIM, 24, BLK), f32),
            pltpu.VMEM((blocks, 24, BLK), f32),
            pltpu.VMEM((8, BLK), f32),
            pltpu.VMEM((n_sub, 8, BLK), f32),
            pltpu.VMEM((8, BLK), f32),
            pltpu.VMEM((n_dom, 8, BLK), f32),
            pltpu.VMEM((n_sub, 5, capacity, BLK), f32),
            pltpu.VMEM((n_sub, 5, capacity, BLK), f32),
            pltpu.VMEM((5, RIM, BLK), f32),
            pltpu.VMEM((5, RIM, BLK), f32),
            pltpu.VMEM((5, blocks, BLK), f32),
            pltpu.VMEM((padded, BLK), i32),
            pltpu.VMEM((padded, BLK), i32),
            pltpu.VMEM((padded, BLK), i32),
            pltpu.VMEM((padded, BLK), i32),
            pltpu.VMEM((2, padded, BLK), f32),
            pltpu.VMEM((6, padded, BLK), f32),
            pltpu.VMEM((padded, BLK), f32),
            pltpu.VMEM((20, padded, BLK), f32),
            pltpu.VMEM((20, padded, BLK), f32),
            pltpu.VMEM((5 * PIECES, padded, BLK), f32),
            sem((n_sub,)),
            sem((n_sub,)),
            sem,
            sem,
            sem((n_sub,)),
            sem((n_sub,)),
            sem((n_dom,)),
            sem((n_dom,)),
            sem((n_sub,)),
            sem((n_sub,)),
            sem,
            sem,
        ],
        compiler_params=pltpu.CompilerParams(collective_id=0, has_side_effects=True),
        name="hydro_step",
    )(
        send_list,
        *operands,
    )
    return rate.reshape(5, cells), new.reshape(5, cells), step.reshape(())


def solution(mesh):
    both = ("dom", "sub")
    wide, flat = P(None, both), P(both)
    in_specs = (wide, wide, flat, flat, flat, wide, flat, wide, flat, flat, wide, flat, wide, flat)
    out_specs = (wide, wide, P())
    step = functools.partial(body, (mesh.shape["dom"], mesh.shape["sub"]))
    return jax.shard_map(step, mesh=mesh, in_specs=in_specs, out_specs=out_specs, check_vma=False)
```

```python
import functools
import jax
import jax.numpy as jnp
from jax import lax
from jax.experimental import pallas as pl
from jax.experimental.pallas import tpu as pltpu
from jax.sharding import PartitionSpec as P

BLK = 128
RIM = 4
GROUP = 13
PIECES = 2

adiabatic = 5.0 / 3.0
courant = 0.3
MESH = pl.DeviceIdType.MESH


def side_state(q, offsets):
    def value(c):
        slopes = q(5 + 3 * c) * offsets[0] + q(6 + 3 * c) * offsets[1] + q(7 + 3 * c) * offsets[2]
        return q(c) + slopes

    return jnp.exp(value(0)), [value(1), value(2), value(3)], jnp.exp(value(4))


def conserved_flux(density, velocity, pressure, normal):
    speed = velocity[0] * normal[0] + velocity[1] * normal[1] + velocity[2] * normal[2]
    square = velocity[0] * velocity[0] + velocity[1] * velocity[1] + velocity[2] * velocity[2]
    energy = pressure / (adiabatic - 1.0) + 0.5 * density * square
    momentum = [density * v for v in velocity]
    conserved = [density] + momentum + [energy]
    flux = (
        [density * speed]
        + [m * speed + pressure * n for m, n in zip(momentum, normal)]
        + [(energy + pressure) * speed]
    )
    return speed, energy, conserved, flux


def star_flux(density, velocity, pressure, normal, speed, energy, conserved, flux, signal, contact, mass_rate):
    factor = mass_rate / (signal - contact)
    jump = contact - speed
    star = (
        [factor]
        + [factor * (v + jump * n) for v, n in zip(velocity, normal)]
        + [factor * (energy / density + jump * (contact + pressure / mass_rate))]
    )
    return [f + signal * (s - u) for f, s, u in zip(flux, star, conserved)]


def hllc(left, right, angles, offsets):
    sin_a = jnp.sin(angles[0])
    normal = [sin_a * jnp.cos(angles[1]), sin_a * jnp.sin(angles[1]), jnp.cos(angles[0])]
    dl, vl, pl_ = side_state(left, offsets[:3])
    dr, vr, pr = side_state(right, offsets[3:])
    ul, el, cl, fl = conserved_flux(dl, vl, pl_, normal)
    ur, er, cr, fr = conserved_flux(dr, vr, pr, normal)
    sound_l = jnp.sqrt(adiabatic * pl_ / dl)
    sound_r = jnp.sqrt(adiabatic * pr / dr)
    signal_l = jnp.minimum(ul - sound_l, ur - sound_r)
    signal_r = jnp.maximum(ul + sound_l, ur + sound_r)
    mass_l = dl * (signal_l - ul)
    mass_r = dr * (signal_r - ur)
    contact = (pr - pl_ + mass_l * ul - mass_r * ur) / (mass_l - mass_r)
    star_l = star_flux(dl, vl, pl_, normal, ul, el, cl, fl, signal_l, contact, mass_l)
    star_r = star_flux(dr, vr, pr, normal, ur, er, cr, fr, signal_r, contact, mass_r)
    out = []
    for a, b, c, d in zip(fl, star_l, star_r, fr):
        inner = jnp.where(contact >= 0, b, jnp.where(signal_r > 0, c, d))
        out.append(jnp.where(signal_l >= 0, a, inner))
    return out


def lane_gather(row, index):
    table = jnp.broadcast_to(row, index.shape)
    return jnp.take_along_axis(table, index, axis=1, mode="promise_in_bounds")


def kernel(dims, send_list, *refs):
    staged = refs[16:29]
    stage_sem = refs[29]
    loads = [pltpu.make_async_copy(source, staged[k], stage_sem.at[k]) for k, source in enumerate(refs[:13])]
    step(dims, send_list, loads, *staged, *refs[13:16], *refs[30:])


def step(
    dims,
    send_list,
    loads,
    prim,
    grad,
    volume,
    face_left,
    face_right,
    face_angles,
    face_area,
    face_offsets,
    rim_left,
    rim_right,
    rim_angles,
    rim_area,
    rim_offsets,
    rate_out,
    new_out,
    step_out,
    outgoing,
    ghosts,
    following,
    table,
    min_own,
    min_sub,
    min_group,
    min_dom,
    gback_send,
    gback_recv,
    rback_send,
    rback_recv,
    cells,
    hi_left,
    lo_left,
    hi_right,
    lo_right,
    angles,
    offsets,
    area,
    gathered_l,
    gathered_r,
    pieces,
    ghost_send_sem,
    ghost_recv_sem,
    rim_send_sem,
    rim_recv_sem,
    min_send_sem,
    min_recv_sem,
    dmin_send_sem,
    dmin_recv_sem,
    gback_send_sem,
    gback_recv_sem,
    rback_send_sem,
    rback_recv_sem,
):
    n_dom, n_sub, capacity, blocks, face_rows = dims
    rows = face_rows + RIM
    group = max(k for k in range(1, GROUP + 1) if rows % k == 0)
    ghost_blocks = n_sub * capacity
    me_dom = lax.axis_index("dom")
    me_sub = lax.axis_index("sub")
    before = lax.rem(me_dom + n_dom - 1, n_dom)
    after = lax.rem(me_dom + 1, n_dom)

    def sub_peer(off):
        return lax.rem(me_sub + off, n_sub)

    def dom_peer(off):
        return lax.rem(me_dom + off, n_dom)

    barrier = pltpu.get_barrier_semaphore()
    for off in range(1, n_sub):
        pl.semaphore_signal(barrier, inc=1, device_id=(me_dom, sub_peer(off)), device_id_type=MESH)
    for off in range(1, n_dom):
        pl.semaphore_signal(barrier, inc=1, device_id=(dom_peer(off), me_sub), device_id_type=MESH)

    for load in loads:
        load.start()
    for k in (0, 1):
        loads[k].wait()

    for h in range(blocks):
        table[h, 0:5, :] = prim[:, h * BLK : (h + 1) * BLK]
        table[h, 5:8, :] = jnp.zeros((3, BLK), jnp.float32)
        table[h, 8:23, :] = grad[:, h * BLK : (h + 1) * BLK]
        table[h, 23:24, :] = jnp.zeros((1, BLK), jnp.float32)

    for off in range(1, n_sub):
        for j in range(capacity):
            block = jnp.maximum(send_list[sub_peer(off) * capacity + j], 0)
            outgoing[off, j] = table[block]

    for k in range(2, len(loads)):
        loads[k].wait()

    for r in range(5):
        for h in range(blocks):
            cells[r, h : h + 1, :] = prim[r : r + 1, h * BLK : (h + 1) * BLK]
    density = jnp.exp(cells[0])
    pressure = jnp.exp(cells[4])
    square = cells[1] * cells[1] + cells[2] * cells[2] + cells[3] * cells[3]
    signal = jnp.sqrt(adiabatic * pressure / density) + jnp.sqrt(square)
    limit = jnp.exp(jnp.log(volume[...]) * (1.0 / 3.0)) / signal
    local_min = jnp.min(limit)
    min_own[...] = jnp.full(min_own.shape, local_min, jnp.float32)

    hi_left[0:face_rows, :] = face_left[...] // BLK
    lo_left[0:face_rows, :] = lax.rem(face_left[...], BLK)
    hi_right[0:face_rows, :] = face_right[...] // BLK
    lo_right[0:face_rows, :] = lax.rem(face_right[...], BLK)
    area[0:face_rows, :] = face_area[...]
    twice = lambda ref: jnp.concatenate([ref[...], ref[...]], 0)
    hi_left[face_rows : face_rows + 8, :] = twice(rim_left) // BLK + (blocks - RIM)
    lo_left[face_rows : face_rows + 8, :] = lax.rem(twice(rim_left), BLK)
    hi_right[face_rows : face_rows + 8, :] = twice(rim_right) // BLK + (blocks + ghost_blocks)
    lo_right[face_rows : face_rows + 8, :] = lax.rem(twice(rim_right), BLK)
    last = me_dom == n_dom - 1
    area[face_rows : face_rows + 8, :] = twice(rim_area)
    for s in range(face_rows):
        for r in range(2):
            angles[r, s : s + 1, :] = face_angles[r : r + 1, s * BLK : (s + 1) * BLK]
        for r in range(6):
            offsets[r, s : s + 1, :] = face_offsets[r : r + 1, s * BLK : (s + 1) * BLK]
    for s in range(8):
        t = s % RIM
        for r in range(2):
            angles[r, face_rows + s : face_rows + s + 1, :] = rim_angles[r : r + 1, t * BLK : (t + 1) * BLK]
        for r in range(6):
            offsets[r, face_rows + s : face_rows + s + 1, :] = rim_offsets[r : r + 1, t * BLK : (t + 1) * BLK]

    tail = pl.ds(face_rows, 8)

    fields = list(range(5)) + list(range(8, 23))

    def gather(hi, lo, entries, names, start):
        match = [hi == name for name in names]
        out = []
        for c, place in enumerate(fields):
            value = start(c)
            for entry, hit in zip(entries, match):
                row = entry[place : place + 1, :]
                value = jnp.where(hit, lane_gather(row, lo), value)
            out.append(value)
        return out

    def gather_into(target, hi, lo, here, entries, names, keep):
        start = (lambda c: target[c, here, :]) if keep else (lambda c: jnp.zeros((8, BLK), jnp.float32))
        for c, value in enumerate(gather(hi[here, :], lo[here, :], entries, names, start)):
            target[c, here, :] = value

    def gather_main(target, hi, lo, entries, names, keep, low=0, high=face_rows // 8):
        def one(g, carry):
            here = pl.ds(pl.multiple_of(g * 8, 8), 8)
            gather_into(target, hi, lo, here, entries, names, keep)
            return carry

        lax.fori_loop(low, high, one, 0)

    own = [table.at[h] for h in range(blocks)]
    gather_main(gathered_l, hi_left, lo_left, own, range(blocks), False)
    gather_main(gathered_r, hi_right, lo_right, own, range(blocks), False, 0, 1)

    pl.semaphore_wait(barrier, n_sub - 1 + n_dom - 1)

    copies = []

    def ghost_copy(off):
        return pltpu.make_async_remote_copy(
            src_ref=outgoing.at[off],
            dst_ref=ghosts.at[off],
            send_sem=ghost_send_sem.at[off],
            recv_sem=ghost_recv_sem.at[off],
            device_id=(me_dom, sub_peer(off)),
            device_id_type=MESH,
        )

    ghost_copies = [ghost_copy(off) for off in range(1, n_sub)]
    for copy in ghost_copies:
        copy.start()
    rim_copy = pltpu.make_async_remote_copy(
        src_ref=table.at[0:RIM],
        dst_ref=following,
        send_sem=rim_send_sem,
        recv_sem=rim_recv_sem,
        device_id=(before, me_sub),
        device_id_type=MESH,
    )
    rim_copy.start()
    min_copies = [
        pltpu.make_async_remote_copy(
            src_ref=min_own,
            dst_ref=min_sub.at[off],
            send_sem=min_send_sem.at[off],
            recv_sem=min_recv_sem.at[off],
            device_id=(me_dom, sub_peer(off)),
            device_id_type=MESH,
        )
        for off in range(1, n_sub)
    ]
    for copy in min_copies:
        copy.start()

    gather_into(gathered_l, hi_left, lo_left, tail, own[blocks - RIM :], range(blocks - RIM, blocks), False)
    gather_main(gathered_r, hi_right, lo_right, own, range(blocks), False, 1)

    for copy in min_copies:
        copy.wait()
    group_min = min_own[...]
    for off in range(1, n_sub):
        group_min = jnp.minimum(group_min, min_sub[off])
    min_group[...] = group_min

    rim_copy.wait()

    first = blocks + ghost_blocks
    nexts = [following.at[h] for h in range(RIM)]
    gather_into(gathered_r, hi_right, lo_right, tail, nexts, range(first, first + RIM), False)

    dmin_copies = [
        pltpu.make_async_remote_copy(
            src_ref=min_group,
            dst_ref=min_dom.at[off],
            send_sem=dmin_send_sem.at[off],
            recv_sem=dmin_recv_sem.at[off],
            device_id=(dom_peer(off), me_sub),
            device_id_type=MESH,
        )
        for off in range(1, n_dom)
    ]
    for copy in dmin_copies:
        copy.start()

    for copy in ghost_copies:
        copy.wait()

    entries, names = [], []
    for off in range(1, n_sub):
        sender = lax.rem(me_sub + n_sub - off, n_sub)
        for j in range(capacity):
            entries.append(ghosts.at[off, j])
            names.append(blocks + sender * capacity + j)
    gather_main(gathered_r, hi_right, lo_right, entries, names, True)

    def flux_step(g, carry):
        here = pl.ds(pl.multiple_of(g * 8, 8), 8)
        flux = hllc(
            lambda c: gathered_l[c, here, :],
            lambda c: gathered_r[c, here, :],
            [angles[k, here, :] for k in range(2)],
            [offsets[k, here, :] for k in range(6)],
        )
        idle = jnp.logical_and(g * 8 >= face_rows, last)
        for c in range(5):
            value = jnp.where(idle, 0.0, flux[c] * area[here, :])
            big = value.astype(jnp.bfloat16).astype(jnp.float32)
            pieces[c, here, :] = big
            pieces[5 + c, here, :] = value - big
        return carry

    lax.fori_loop(0, (face_rows + 8) // 8, flux_step, 0, unroll=True)

    lane_iota = lax.broadcasted_iota(jnp.int32, (BLK, BLK), 0)

    def one_hot(lo, s):
        return jnp.where(lane_iota == lo[pl.ds(s, 1), :], 1.0, 0.0).astype(jnp.bfloat16)

    def spread(hi, s, first, count, sign):
        place = lax.broadcasted_iota(jnp.int32, (count, BLK), 0) + first
        match = place == hi[pl.ds(s, 1), :]
        parts = []
        for c in range(5 * PIECES):
            value = pieces[c, pl.ds(s, 1), :]
            value = value if sign > 0 else -value
            parts.append(jnp.where(match, value, 0.0))
        return jnp.concatenate(parts, 0).astype(jnp.bfloat16)

    def product(a, b):
        return lax.dot_general(a, b, (((1,), (1,)), ((), ())), preferred_element_type=jnp.float32)

    def fold(total, count):
        total = total.reshape(PIECES, 5, count, BLK)
        return total[0] + total[1]

    away = -(-(ghost_blocks + RIM) // 8) * 8

    def away_step(i, total):
        a = jnp.concatenate([spread(hi_right, i * group + k, blocks, away, -1) for k in range(group)], 1)
        b = jnp.concatenate([one_hot(lo_right, i * group + k) for k in range(group)], 1)
        return total + product(a, b)

    total = lax.fori_loop(0, rows // group, away_step, jnp.zeros((5 * PIECES * away, BLK), jnp.float32))
    total = fold(total, away)
    for s in range(n_sub):
        gback_send[s] = total[:, s * capacity : (s + 1) * capacity, :]
    rback_send[...] = total[:, ghost_blocks : ghost_blocks + RIM, :]
    gback_copies = [
        pltpu.make_async_remote_copy(
            src_ref=gback_send.at[sub_peer(off)],
            dst_ref=gback_recv.at[off],
            send_sem=gback_send_sem.at[off],
            recv_sem=gback_recv_sem.at[off],
            device_id=(me_dom, sub_peer(off)),
            device_id_type=MESH,
        )
        for off in range(1, n_sub)
    ]
    for copy in gback_copies:
        copy.start()
    rback_copy = pltpu.make_async_remote_copy(
        src_ref=rback_send,
        dst_ref=rback_recv,
        send_sem=rback_send_sem,
        recv_sem=rback_recv_sem,
        device_id=(after, me_sub),
        device_id_type=MESH,
    )
    rback_copy.start()

    def local_step(i, total):
        a = [spread(hi_left, i * group + k, 0, blocks, 1) for k in range(group)]
        a += [spread(hi_right, i * group + k, 0, blocks, -1) for k in range(group)]
        b = [one_hot(lo_left, i * group + k) for k in range(group)]
        b += [one_hot(lo_right, i * group + k) for k in range(group)]
        return total + product(jnp.concatenate(a, 1), jnp.concatenate(b, 1))

    total = lax.fori_loop(0, rows // group, local_step, jnp.zeros((5 * PIECES * blocks, BLK), jnp.float32))
    net = fold(total, blocks)

    for copy in dmin_copies:
        copy.wait()
    smallest = min_group[...]
    for off in range(1, n_dom):
        smallest = jnp.minimum(smallest, min_dom[off])
    time_step = courant * smallest
    step_out[0] = jnp.min(time_step)
    time_step = time_step[0:1, :]

    rback_copy.wait()
    for copy in gback_copies:
        copy.wait()

    place = lax.broadcasted_iota(jnp.int32, (blocks, BLK), 0)
    density = jnp.exp(cells[0])
    pressure = jnp.exp(cells[4])
    square = cells[1] * cells[1] + cells[2] * cells[2] + cells[3] * cells[3]
    energy = pressure / (adiabatic - 1.0) + 0.5 * density * square
    conserved = [density, density * cells[1], density * cells[2], density * cells[3], energy]
    for c in range(5):
        sums = net[c]
        for h in range(RIM):
            sums = sums + jnp.where(place == h, rback_recv[c, h : h + 1, :], 0.0)
        for off in range(1, n_sub):
            sender = lax.rem(me_sub + n_sub - off, n_sub)
            for j in range(capacity):
                wanted = send_list[sender * capacity + j]
                sums = sums + jnp.where(place == wanted, gback_recv[off, c, j : j + 1, :], 0.0)
        rate = -sums / volume[...]
        rate_out[c] = rate
        new_out[c] = conserved[c] + time_step * rate


def body(mesh_sizes, *args):
    (primitive, gradient, volume, face_left, face_right, face_angles, face_area, face_offsets) = args[:8]
    (rim_left, rim_right, rim_angles, rim_area, rim_offsets, send_list) = args[8:]
    n_dom, n_sub = mesh_sizes
    cells = primitive.shape[1]
    blocks = cells // BLK
    face_rows = face_left.shape[0] // BLK
    capacity = send_list.shape[0] // n_sub
    padded = face_rows + 8
    dims = (n_dom, n_sub, capacity, blocks, face_rows)
    f32, i32 = jnp.float32, jnp.int32
    vmem = pl.BlockSpec(memory_space=pltpu.VMEM)
    smem = pl.BlockSpec(memory_space=pltpu.SMEM)
    sem = pltpu.SemaphoreType.DMA
    operands = (
        primitive,
        gradient,
        volume.reshape(blocks, BLK),
        face_left.reshape(face_rows, BLK),
        face_right.reshape(face_rows, BLK),
        face_angles,
        face_area.reshape(face_rows, BLK),
        face_offsets,
        rim_left.reshape(RIM, BLK),
        rim_right.reshape(RIM, BLK),
        rim_angles,
        rim_area.reshape(RIM, BLK),
        rim_offsets,
    )
    rate, new, step = pl.pallas_call(
        functools.partial(kernel, dims),
        out_shape=(
            jax.ShapeDtypeStruct((5, blocks, BLK), f32),
            jax.ShapeDtypeStruct((5, blocks, BLK), f32),
            jax.ShapeDtypeStruct((1,), f32),
        ),
        in_specs=[smem] + [pl.BlockSpec(memory_space=pl.ANY)] * 13,
        out_specs=(vmem, vmem, smem),
        scratch_shapes=[pltpu.VMEM(x.shape, x.dtype) for x in operands]
        + [
            sem((len(operands),)),
            pltpu.VMEM((n_sub, capacity, 24, BLK), f32),
            pltpu.VMEM((n_sub, capacity, 24, BLK), f32),
            pltpu.VMEM((RIM, 24, BLK), f32),
            pltpu.VMEM((blocks, 24, BLK), f32),
            pltpu.VMEM((8, BLK), f32),
            pltpu.VMEM((n_sub, 8, BLK), f32),
            pltpu.VMEM((8, BLK), f32),
            pltpu.VMEM((n_dom, 8, BLK), f32),
            pltpu.VMEM((n_sub, 5, capacity, BLK), f32),
            pltpu.VMEM((n_sub, 5, capacity, BLK), f32),
            pltpu.VMEM((5, RIM, BLK), f32),
            pltpu.VMEM((5, RIM, BLK), f32),
            pltpu.VMEM((5, blocks, BLK), f32),
            pltpu.VMEM((padded, BLK), i32),
            pltpu.VMEM((padded, BLK), i32),
            pltpu.VMEM((padded, BLK), i32),
            pltpu.VMEM((padded, BLK), i32),
            pltpu.VMEM((2, padded, BLK), f32),
            pltpu.VMEM((6, padded, BLK), f32),
            pltpu.VMEM((padded, BLK), f32),
            pltpu.VMEM((20, padded, BLK), f32),
            pltpu.VMEM((20, padded, BLK), f32),
            pltpu.VMEM((5 * PIECES, padded, BLK), f32),
            sem((n_sub,)),
            sem((n_sub,)),
            sem,
            sem,
            sem((n_sub,)),
            sem((n_sub,)),
            sem((n_dom,)),
            sem((n_dom,)),
            sem((n_sub,)),
            sem((n_sub,)),
            sem,
            sem,
        ],
        compiler_params=pltpu.CompilerParams(collective_id=0, has_side_effects=True),
        name="hydro_step",
    )(
        send_list,
        *operands,
    )
    return rate.reshape(5, cells), new.reshape(5, cells), step.reshape(())


def solution(mesh):
    both = ("dom", "sub")
    wide, flat = P(None, both), P(both)
    in_specs = (wide, wide, flat, flat, flat, wide, flat, wide, flat, flat, wide, flat, wide, flat)
    out_specs = (wide, wide, P())
    step = functools.partial(body, (mesh.shape["dom"], mesh.shape["sub"]))
    return jax.shard_map(step, mesh=mesh, in_specs=in_specs, out_specs=out_specs, check_vma=False)
```
